32 devices in a mesh: chain: 4 (over z), inner: 8 (over y, x, core).
Axes of the slice: x: 2, y: 2, z: 4, core: 2. Of those that a mesh axis runs over, the one named last changes fastest.
Arguments:
- queries: bfloat16 [4096, 4096], P(('chain', 'inner')), may hold values from -0.75 to 0.75
- key_rows: bfloat16 [4096, 4096], P(('chain', 'inner')), may hold values from -0.75 to 0.75
- value_rows: bfloat16 [4096, 4096], P(('chain', 'inner')), may hold values from -0.75 to 0.75
- out_grad: bfloat16 [4096, 4096], P(('chain', 'inner')), may hold values from -0.75 to 0.75
- log_decay: bfloat16 [4096, 32], P(('chain', 'inner')), may hold values from -2 to 0, as said below
Outputs:
- attended: bfloat16 [4096, 4096], P(('chain', 'inner'))
- query_grad: bfloat16 [4096, 4096], P(('chain', 'inner'))
- key_grad: bfloat16 [4096, 4096], P(('chain', 'inner'))
- value_grad: bfloat16 [4096, 4096], P(('chain', 'inner'))
The draws below stay inside these ranges and needn't reach their ends.
Inputs may be any that keep to these rules, and one draw needn't show every extreme that they name: `log_decay`: every entry is negative.
All inputs are finite; a program needn't handle non-finite values.
Results may differ from the reference program's by a relative error of at most 0.0051.
Values may be sent and summed in bfloat16 or wider, within the bound.
A program may use at most 64 MiB of HBM per device.

```python
import jax
import jax.numpy as jnp
from jax import lax

HEAD_SIZE = 128
HEAD_COUNT = 32
BLOCK = 128
TOKEN_COUNT = 4096


def draw_log_decay(key, part):
    parallel_sequences = jax.random.split(key, 5)
    quick_heads = jax.random.randint(parallel_sequences[0], (HEAD_COUNT,), 0, 2) == 1
    spread = jnp.exp(jax.random.uniform(parallel_sequences[1], (HEAD_COUNT,), minval=-0.69, maxval=0.69))
    head_decay_speeds = jnp.where(quick_heads, 3.0 / BLOCK, 0.15 / TOKEN_COUNT) * spread
    decay_jitter = jax.random.uniform(parallel_sequences[2], (TOKEN_COUNT, HEAD_COUNT), minval=0.5, maxval=2.0)
    spike_token_rows = jax.random.randint(parallel_sequences[3], (3,), 0, TOKEN_COUNT)
    spike_length = jnp.log(jax.random.uniform(parallel_sequences[4], (3, HEAD_COUNT), minval=0.55, maxval=0.8))
    spike_positions = (jnp.arange(TOKEN_COUNT)[:, None] == spike_token_rows[None, :]).astype(jnp.float32)
    value_inputs = -(head_decay_speeds[None, :] * decay_jitter) + jnp.dot(spike_positions, spike_length)
    return value_inputs.astype(jnp.bfloat16)


def levels(own_key, dims, cuts, least, high):
    level, own = 1.0, jax.random.fold_in(own_key, 6)
    for axis_at, blocks in cuts:
        draws = jnp.exp(jax.random.uniform(jax.random.fold_in(own, axis_at), (blocks,), jnp.float32, least / len(cuts), high / len(cuts)))
        level = level * jnp.repeat(draws, dims[axis_at] // blocks).reshape([-1 if axis == axis_at else 1 for axis in range(len(dims))])
    return level


def bell_draw(rng, dims, width, limit, pieces=(), held_as=jnp.bfloat16):
    drawn = jax.random.normal(rng, dims, jnp.float32) * width
    if len(pieces) > 0:
        drawn = levels(rng, dims, pieces, -0.22, 0.18) * drawn
    return jnp.clip(drawn, min=-limit, max=limit).astype(held_as)


def setup_inputs(seed: int = 0) -> dict:
    key_of = jax.random.split(jax.random.key(seed), 6)
    return {
        "queries": bell_draw(key_of[0], (TOKEN_COUNT, HEAD_COUNT * HEAD_SIZE), 0.125, 0.75, ((0, 32),)),
        "key_rows": bell_draw(key_of[1], (TOKEN_COUNT, HEAD_COUNT * HEAD_SIZE), 0.125, 0.75, ((0, 32),)),
        "value_rows": bell_draw(key_of[2], (TOKEN_COUNT, HEAD_COUNT * HEAD_SIZE), 0.125, 0.75, ((0, 32),)),
        "out_grad": bell_draw(key_of[3], (TOKEN_COUNT, HEAD_COUNT * HEAD_SIZE), 0.125, 0.75, ((0, 32),)),
        "log_decay": draw_log_decay(jax.random.fold_in(key_of[5], 71), 0),
    }


def advance(state, inputs):
    factor, term = inputs
    return jnp.exp(factor) * state + term, state


def narrowed(array):
    return lax.optimization_barrier(array.astype(jnp.bfloat16)).astype(jnp.float32)


def one_head(query_head, key_head, value_head, grad_head, decay_head):
    blocks = TOKEN_COUNT // BLOCK
    highest = lax.Precision.HIGHEST
    query_f = query_head.astype(jnp.float32).reshape(blocks, BLOCK, HEAD_SIZE)
    key_f = key_head.astype(jnp.float32).reshape(blocks, BLOCK, HEAD_SIZE)
    value_f = value_head.astype(jnp.float32).reshape(blocks, BLOCK, HEAD_SIZE)
    grad_f = grad_head.astype(jnp.float32).reshape(blocks, BLOCK, HEAD_SIZE)
    cumul = jnp.cumsum(decay_head.astype(jnp.float32).reshape(blocks, BLOCK), axis=1)
    finals = cumul[:, -1]
    forward_scale = jnp.exp(cumul)[:, :, None]
    backward_scale = jnp.exp(finals[:, None] - cumul)[:, :, None]
    scaled_keys = narrowed(key_f * backward_scale)
    scaled_queries = narrowed(query_f * forward_scale)
    kv_terms = jnp.einsum("jsd,jse->jde", scaled_keys, value_f, precision=highest)
    qd_terms = jnp.einsum("jtd,jte->jde", scaled_queries, grad_f, precision=highest)
    zero_state = jnp.zeros((HEAD_SIZE, HEAD_SIZE), jnp.float32)
    _, entering = lax.scan(advance, zero_state, (finals, kv_terms))
    _, trailing = lax.scan(advance, zero_state, (finals, qd_terms), reverse=True)
    enter_narrow = narrowed(entering)
    trail_narrow = narrowed(trailing)
    positions = jnp.arange(BLOCK)
    lower = positions[:, None] >= positions[None, :]
    weights = jnp.exp(jnp.where(lower[None], cumul[:, :, None] - cumul[:, None, :], -jnp.inf))
    scores = jnp.einsum("jtd,jsd->jts", query_f, key_f, precision=highest)
    probs = narrowed(scores * weights)
    grows = narrowed(jnp.einsum("jte,jse->jts", grad_f, value_f, precision=highest) * weights)
    attended = jnp.einsum("jts,jse->jte", probs, value_f, precision=highest) + forward_scale * jnp.einsum("jtd,jde->jte", query_f, enter_narrow, precision=highest)
    query_grad = jnp.einsum("jts,jsd->jtd", grows, key_f, precision=highest) + forward_scale * jnp.einsum("jte,jde->jtd", grad_f, enter_narrow, precision=highest)
    key_grad = jnp.einsum("jts,jtd->jsd", grows, query_f, precision=highest) + backward_scale * jnp.einsum("jse,jde->jsd", value_f, trail_narrow, precision=highest)
    value_grad = jnp.einsum("jts,jte->jse", probs, grad_f, precision=highest) + backward_scale * jnp.einsum("jsd,jde->jse", key_f, trail_narrow, precision=highest)
    return tuple(item.reshape(TOKEN_COUNT, HEAD_SIZE).astype(jnp.bfloat16) for item in (attended, query_grad, key_grad, value_grad))


def head_major(array):
    return array.reshape(TOKEN_COUNT, HEAD_COUNT, HEAD_SIZE).transpose(1, 0, 2)


def token_major(array):
    return array.transpose(1, 0, 2).reshape(TOKEN_COUNT, HEAD_COUNT * HEAD_SIZE)


def reference(queries, key_rows, value_rows, out_grad, log_decay):
    stacked = (head_major(queries), head_major(key_rows), head_major(value_rows), head_major(out_grad), log_decay.T)
    results = lax.map(lambda items: one_head(items[0], items[1], items[2], items[3], items[4]), stacked)
    return (token_major(results[0]), token_major(results[1]), token_major(results[2]), token_major(results[3]))
```

```python
import functools

import jax
import jax.numpy as jnp
from jax import lax
from jax.experimental import pallas as pl
from jax.experimental.pallas import tpu as pltpu
from jax.sharding import PartitionSpec as P

SIZE = 128
F32 = jnp.float32
BF16 = jnp.bfloat16
MESH = pl.DeviceIdType.MESH


def triangle(rows):
    row = lax.broadcasted_iota(jnp.int32, (rows, rows), 0)
    column = lax.broadcasted_iota(jnp.int32, (rows, rows), 1)
    return row >= column


def spread_column(decay, head):
    rows, heads = decay.shape
    pick = (lax.broadcasted_iota(jnp.int32, (heads, SIZE), 0) == head).astype(F32).astype(BF16)
    column = jnp.dot(decay, pick, preferred_element_type=F32).astype(BF16)
    lower = triangle(rows).astype(F32).astype(BF16)
    return jnp.dot(lower, column, preferred_element_type=F32), column


def over_rows(left, right):
    return lax.dot_general(left, right, (((0,), (0,)), ((), ())), preferred_element_type=F32)


def over_columns(left, right):
    return lax.dot_general(left, right, (((1,), (1,)), ((), ())), preferred_element_type=F32)


def states_kernel(
    planes, devices, q_ref, k_ref, v_ref, g_ref, decay_ref, states_ref,
    terms, from_core, to_chips, from_chips, plane_sum, from_planes, to_back, from_back, to_core,
    own_fin, core_fin, chip_fin, plane_fin,
    fin_s, fin_r, chip_fs, chip_fr, plane_fs, plane_fr,
    core_s, core_r, out_s, out_r, plane_s, plane_r, back_s, back_r, last_s, last_r,
):
    rows, heads = decay_ref.shape
    chips = devices // 2
    own = heads // devices
    z = lax.axis_index("chain")
    me = lax.axis_index("inner")
    chip, core = me // 2, lax.rem(me, 2)
    first_core = core == 0

    def at_core():
        return (z, chip * 2 + 1 - core)

    def at_chip(other):
        return (z, other * 2 + core)

    def at_plane(other):
        return (other, me)

    def remote(src, dst, send, recv, to):
        return pltpu.make_async_remote_copy(
            src_ref=src, dst_ref=dst, send_sem=send, recv_sem=recv, device_id=to, device_id_type=MESH
        )

    barrier = pltpu.get_barrier_semaphore()
    pl.semaphore_signal(barrier, inc=1, device_id=at_core(), device_id_type=MESH)
    for step in range(1, chips):
        pl.semaphore_signal(
            barrier, inc=1, device_id=at_chip(lax.rem(chip + step, chips)), device_id_type=MESH
        )
    for step in range(1, planes):
        pl.semaphore_signal(
            barrier, inc=1, device_id=at_plane(lax.rem(z + step, planes)), device_id_type=MESH
        )

    decay = decay_ref[...]
    own_fin[...] = over_rows(decay, jnp.ones((rows, SIZE), BF16))
    from_planes[z] = jnp.zeros(from_planes.shape[1:], BF16)
    pl.semaphore_wait(barrier, chips + planes - 1)

    fin_copy = remote(own_fin, core_fin, fin_s, fin_r, at_core())
    fin_copy.start()

    def make_terms(head):
        cumul, _ = spread_column(decay, head)
        columns = pl.ds(pl.multiple_of(head * SIZE, SIZE), SIZE)
        final = cumul[rows - 1 :, :]
        keys = (k_ref[:, columns].astype(F32) * jnp.exp(final - cumul)).astype(BF16)
        queries = (q_ref[:, columns].astype(F32) * jnp.exp(cumul)).astype(BF16)
        terms[head, 0] = over_rows(keys, v_ref[:, columns]).astype(BF16)
        terms[head, 1] = over_rows(queries, g_ref[:, columns]).astype(BF16)

    def core_copy(i, other):
        slot = other * own + i
        head = (other * 2 + 1 - core) * own + i
        return remote(
            terms.at[head], from_core.at[slot], core_s.at[slot], core_r.at[slot], at_core()
        )

    def first(i):
        @pl.loop(0, chips)
        def _(step):
            other = lax.rem(chip + 1 + step, chips)
            make_terms((other * 2 + 1 - core) * own + i)
            core_copy(i, other).start()

    def out_copy(i, other):
        return remote(
            to_chips.at[other, i], from_chips.at[chip, i], out_s.at[other * own + i],
            out_r.at[chip * own + i], at_chip(other),
        )

    def out_arrival(i, other):
        return remote(
            to_chips.at[other, i], from_chips.at[other, i], out_s.at[other * own + i],
            out_r.at[other * own + i], at_chip(other),
        )

    def second(i):
        @pl.loop(0, chips)
        def _(step):
            other = lax.rem(chip + 1 + step, chips)
            head = (other * 2 + core) * own + i
            make_terms(head)
            core_copy(i, other).wait_recv()
            slot = other * own + i
            mine = jnp.exp(own_fin[pl.ds(head, 1), :])
            theirs = jnp.exp(core_fin[pl.ds(head, 1), :])
            one = jnp.ones_like(mine)
            kv = (
                jnp.where(first_core, theirs, one) * terms[head, 0].astype(F32)
                + jnp.where(first_core, one, mine) * from_core[slot, 0].astype(F32)
            ).astype(BF16)
            qd = (
                jnp.where(first_core, one, theirs) * terms[head, 1].astype(F32)
                + jnp.where(first_core, mine, one) * from_core[slot, 1].astype(F32)
            ).astype(BF16)

            @pl.when(step < chips - 1)
            def _():
                to_chips[other, i, 0] = kv
                to_chips[other, i, 1] = qd
                out_copy(i, other).start()

            @pl.when(step == chips - 1)
            def _():
                from_chips[chip, i, 0] = kv
                from_chips[chip, i, 1] = qd

    first(0)
    fin_copy.wait_recv()
    chip_fin[chip] = own_fin[...] + core_fin[...]

    def chip_fin_copy(other, slot):
        return remote(
            chip_fin.at[chip], chip_fin.at[slot], chip_fs.at[other], chip_fr.at[slot], at_chip(other)
        )

    for step in range(1, chips):
        chip_fin_copy(lax.rem(chip + step, chips), chip).start()

    @pl.loop(0, own - 1)
    def _(i):
        second(i)
        first(i + 1)

    second(own - 1)

    for step in range(1, chips):
        other = lax.rem(chip + step, chips)
        chip_fin_copy(other, other).wait_recv()
    total = chip_fin[0]
    for other in range(1, chips):
        total = total + chip_fin[other]
    plane_fin[z] = total

    def plane_fin_copy(other, slot):
        return remote(
            plane_fin.at[z], plane_fin.at[slot], plane_fs.at[other], plane_fr.at[slot],
            at_plane(other),
        )

    for step in range(1, planes):
        plane_fin_copy(lax.rem(z + step, planes), z).start()

    def plane_copy(i, other, slot):
        kind = jnp.where(other > z, 0, 1)
        return remote(
            plane_sum.at[i, kind], from_planes.at[slot, i], plane_s.at[other * own + i],
            plane_r.at[slot * own + i], at_plane(other),
        )

    def sum_plane(i):
        head = me * own + i
        for step in range(1, chips):
            out_arrival(i, lax.rem(chip + step, chips)).wait_recv()
        kv = from_chips[0, i, 0].astype(F32)
        qd = from_chips[chips - 1, i, 1].astype(F32)
        for other in range(1, chips):
            kv = kv * jnp.exp(chip_fin[other, pl.ds(head, 1), :]) + from_chips[other, i, 0].astype(F32)
            back = chips - 1 - other
            qd = qd * jnp.exp(chip_fin[back, pl.ds(head, 1), :]) + from_chips[back, i, 1].astype(F32)
        plane_sum[i, 0] = kv.astype(BF16)
        plane_sum[i, 1] = qd.astype(BF16)
        for step in range(1, planes):
            plane_copy(i, lax.rem(z + step, planes), z).start()

    def back_copy(i, other):
        return remote(
            to_back.at[other, i], from_back.at[chip, i], back_s.at[other * own + i],
            back_r.at[chip * own + i], at_chip(other),
        )

    def back_arrival(i, other):
        return remote(
            to_back.at[other, i], from_back.at[other, i], back_s.at[other * own + i],
            back_r.at[other * own + i], at_chip(other),
        )

    def carry(i):
        head = me * own + i
        for step in range(1, planes):
            other = lax.rem(z + step, planes)
            plane_copy(i, other, other).wait_recv()
        kv = jnp.zeros((SIZE, SIZE), F32)
        qd = jnp.zeros((SIZE, SIZE), F32)
        for other in range(planes):
            factor = jnp.exp(plane_fin[other, pl.ds(head, 1), :])
            kv = jnp.where(other < z, kv * factor + from_planes[other, i].astype(F32), kv)
            back = planes - 1 - other
            factor = jnp.exp(plane_fin[back, pl.ds(head, 1), :])
            qd = jnp.where(back > z, qd * factor + from_planes[back, i].astype(F32), qd)
        for other in range(chips):
            to_back[other, i, 0] = kv.astype(BF16)
            back = chips - 1 - other
            to_back[back, i, 1] = qd.astype(BF16)
            if other < chips - 1:
                factor = jnp.exp(chip_fin[other, pl.ds(head, 1), :])
                kv = kv * factor + from_chips[other, i, 0].astype(F32)
                factor = jnp.exp(chip_fin[back, pl.ds(head, 1), :])
                qd = qd * factor + from_chips[back, i, 1].astype(F32)
        for step in range(1, chips):
            back_copy(i, lax.rem(chip + step, chips)).start()
        from_back[chip, i] = to_back[chip, i]

    def last_copy(i, other, side):
        head = (other * 2 + side) * own + i
        slot = other * own + i
        return remote(
            to_core.at[slot], states_ref.at[head], last_s.at[slot], last_r.at[slot], at_core()
        )

    def finish(i):
        @pl.loop(0, chips)
        def _(step):
            other = lax.rem(chip + step, chips)

            @pl.when(step > 0)
            def _():
                back_arrival(i, other).wait_recv()

            head = (other * 2 + core) * own + i
            slot = other * own + i
            mine = jnp.exp(own_fin[pl.ds(head, 1), :])
            theirs = jnp.exp(core_fin[pl.ds(head, 1), :])
            one = jnp.ones_like(mine)
            enter = from_back[other, i, 0].astype(F32)
            trail = from_back[other, i, 1].astype(F32)
            late = jnp.where(
                first_core, mine * enter + terms[head, 0].astype(F32),
                theirs * enter + from_core[slot, 0].astype(F32),
            )
            early = jnp.where(
                first_core, theirs * trail + from_core[slot, 1].astype(F32),
                mine * trail + terms[head, 1].astype(F32),
            )
            to_core[slot, 0] = jnp.where(first_core, late, enter).astype(BF16)
            to_core[slot, 1] = jnp.where(first_core, trail, early).astype(BF16)
            last_copy(i, other, core).start()
            states_ref[head, 0] = jnp.where(first_core, enter, late).astype(BF16)
            states_ref[head, 1] = jnp.where(first_core, early, trail).astype(BF16)

    lead = min(3, own)
    pl.loop(0, lead)(sum_plane)
    for step in range(1, planes):
        other = lax.rem(z + step, planes)
        plane_fin_copy(other, other).wait_recv()

    @pl.loop(0, own - lead)
    def _(i):
        carry(i)
        sum_plane(i + lead)

    pl.loop(own - lead, own)(carry)
    pl.loop(0, own)(finish)

    fin_copy.wait_send()
    for step in range(1, chips):
        chip_fin_copy(lax.rem(chip + step, chips), chip).wait_send()
    for step in range(1, planes):
        plane_fin_copy(lax.rem(z + step, planes), z).wait_send()

    @pl.loop(0, own)
    def _(i):
        @pl.loop(0, chips)
        def _(other):
            core_copy(i, other).wait_send()
            last_copy(i, other, core).wait_send()
            last_copy(i, other, 1 - core).wait_recv()

        @pl.loop(1, chips)
        def _(step):
            other = lax.rem(chip + step, chips)
            out_copy(i, other).wait_send()
            back_copy(i, other).wait_send()

        @pl.loop(1, planes)
        def _(step):
            plane_copy(i, lax.rem(z + step, planes), z).wait_send()


def carried_states(planes, devices, arrays):
    decay = arrays[-1]
    heads = decay.shape[1]
    chips, own = devices // 2, heads // devices
    square = (SIZE, SIZE)
    dma = pltpu.SemaphoreType.DMA
    slots = chips * own
    return pl.pallas_call(
        functools.partial(states_kernel, planes, devices),
        out_shape=jax.ShapeDtypeStruct((heads, 2) + square, BF16),
        in_specs=[pl.BlockSpec(memory_space=pltpu.VMEM)] * 5,
        out_specs=pl.BlockSpec(memory_space=pltpu.VMEM),
        scratch_shapes=[
            pltpu.VMEM((heads, 2) + square, BF16),
            pltpu.VMEM((slots, 2) + square, BF16),
            pltpu.VMEM((chips, own, 2) + square, BF16),
            pltpu.VMEM((chips, own, 2) + square, BF16),
            pltpu.VMEM((own, 2) + square, BF16),
            pltpu.VMEM((planes, own) + square, BF16),
            pltpu.VMEM((chips, own, 2) + square, BF16),
            pltpu.VMEM((chips, own, 2) + square, BF16),
            pltpu.VMEM((slots, 2) + square, BF16),
            pltpu.VMEM((heads, SIZE), F32),
            pltpu.VMEM((heads, SIZE), F32),
            pltpu.VMEM((chips, heads, SIZE), F32),
            pltpu.VMEM((planes, heads, SIZE), F32),
            dma, dma, dma((chips,)), dma((chips,)), dma((planes,)), dma((planes,)),
            dma((slots,)), dma((slots,)), dma((slots,)), dma((slots,)),
            dma((planes * own,)), dma((planes * own,)),
            dma((slots,)), dma((slots,)), dma((slots,)), dma((slots,)),
        ],
        compiler_params=pltpu.CompilerParams(
            collective_id=0, has_side_effects=True, vmem_limit_bytes=40 * 2**20
        ),
    )(*arrays)


def block_kernel(
    group, q_ref, k_ref, v_ref, g_ref, decay_ref, states_ref, o_ref, dq_ref, dk_ref, dv_ref
):
    decay = decay_ref[...]
    rows = decay.shape[0]
    lower = triangle(rows)
    for i in range(group):
        head = pl.program_id(0) * group + i
        columns = slice(i * SIZE, (i + 1) * SIZE)
        query, key, value, grad = (ref[:, columns] for ref in (q_ref, k_ref, v_ref, g_ref))
        enter, trail = states_ref[i, 0], states_ref[i, 1]
        cumul, column = spread_column(decay, head)
        upper = (
            lax.broadcasted_iota(jnp.int32, (rows, rows), 0)
            <= lax.broadcasted_iota(jnp.int32, (rows, rows), 1)
        ).astype(F32).astype(BF16)
        across = over_rows(column, upper)
        weights = jnp.exp(jnp.where(lower, cumul - across, -jnp.inf))
        forward = jnp.exp(cumul)
        backward = jnp.exp(cumul[rows - 1 :, :] - cumul)
        probs = (over_columns(query, key) * weights).astype(BF16)
        grows = (over_columns(grad, value) * weights).astype(BF16)
        o_ref[:, columns] = (
            jnp.dot(probs, value, preferred_element_type=F32)
            + forward * jnp.dot(query, enter, preferred_element_type=F32)
        ).astype(BF16)
        dq_ref[:, columns] = (
            jnp.dot(grows, key, preferred_element_type=F32) + forward * over_columns(grad, enter)
        ).astype(BF16)
        dk_ref[:, columns] = (
            over_rows(grows, query) + backward * over_columns(value, trail)
        ).astype(BF16)
        dv_ref[:, columns] = (
            over_rows(probs, grad) + backward * jnp.dot(key, trail, preferred_element_type=F32)
        ).astype(BF16)


def block_results(arrays, states):
    rows, heads = arrays[-1].shape
    group = 4
    wide = pl.BlockSpec((rows, group * SIZE), lambda i: (0, i))
    return pl.pallas_call(
        functools.partial(block_kernel, group),
        grid=(heads // group,),
        out_shape=[jax.ShapeDtypeStruct(arrays[0].shape, BF16)] * 4,
        in_specs=[wide] * 4
        + [
            pl.BlockSpec((rows, heads), lambda i: (0, 0)),
            pl.BlockSpec((group, 2, SIZE, SIZE), lambda i: (i, 0, 0, 0)),
        ],
        out_specs=[wide] * 4,
    )(*arrays, states)


def solution(mesh):
    planes, devices = mesh.shape["chain"], mesh.shape["inner"]

    def shards(*arrays):
        return tuple(block_results(arrays, carried_states(planes, devices, arrays)))

    spec = P(("chain", "inner"), None)
    return jax.shard_map(
        shards, mesh=mesh, in_specs=(spec,) * 5, out_specs=(spec,) * 4, check_vma=False
    )
```

```python
import functools

import jax
import jax.numpy as jnp
from jax import lax
from jax.experimental import pallas as pl
from jax.experimental.pallas import tpu as pltpu
from jax.sharding import PartitionSpec as P

SIZE = 128
F32 = jnp.float32
BF16 = jnp.bfloat16
MESH = pl.DeviceIdType.MESH


def triangle(rows):
    row = lax.broadcasted_iota(jnp.int32, (rows, rows), 0)
    column = lax.broadcasted_iota(jnp.int32, (rows, rows), 1)
    return row >= column


def spread_column(decay, head):
    rows, heads = decay.shape
    pick = (lax.broadcasted_iota(jnp.int32, (heads, SIZE), 0) == head).astype(F32).astype(BF16)
    column = jnp.dot(decay, pick, preferred_element_type=F32).astype(BF16)
    lower = triangle(rows).astype(F32).astype(BF16)
    return jnp.dot(lower, column, preferred_element_type=F32)


def over_rows(left, right):
    return lax.dot_general(left, right, (((0,), (0,)), ((), ())), preferred_element_type=F32)


def over_columns(left, right):
    return lax.dot_general(left, right, (((1,), (1,)), ((), ())), preferred_element_type=F32)


def states_kernel(
    planes, devices, q_any, k_any, v_any, g_any, decay_ref, states_ref,
    q_ref, k_ref, v_ref, g_ref, cumuls, local,
    cumul_rows, terms, from_core, to_chips, from_chips, plane_sum, from_planes, to_back, from_back, to_core,
    own_fin, core_fin, chip_fin, plane_fin,
    load_s, fin_s, fin_r, chip_fs, chip_fr, plane_fs, plane_fr,
    core_s, core_r, out_s, out_r, plane_s, plane_r, back_s, back_r, last_s, last_r,
):
    rows, heads = decay_ref.shape
    chips = devices // 2
    own = heads // devices
    z = lax.axis_index("chain")
    me = lax.axis_index("inner")
    chip, core = me // 2, lax.rem(me, 2)
    first_core = core == 0

    def at_core():
        return (z, chip * 2 + 1 - core)

    def at_chip(other):
        return (z, other * 2 + core)

    def at_plane(other):
        return (other, me)

    def remote(src, dst, send, recv, to):
        return pltpu.make_async_remote_copy(
            src_ref=src, dst_ref=dst, send_sem=send, recv_sem=recv, device_id=to, device_id_type=MESH
        )

    def loads(group, part):
        begin, width = (0, SIZE) if part == 0 else (SIZE, (own - 1) * SIZE)
        columns = pl.ds(pl.multiple_of(group * (own * SIZE) + begin, SIZE), width)
        pairs = ((q_any, q_ref), (k_any, k_ref), (v_any, v_ref), (g_any, g_ref))
        return [
            pltpu.make_async_copy(src.at[:, columns], dst.at[:, columns], load_s.at[j, group, part])
            for j, (src, dst) in enumerate(pairs)
        ]

    def owner(step, side):
        return lax.rem(chip + 1 + step, chips) * 2 + side

    for side in (1 - core, core):
        @pl.loop(0, chips)
        def _(step):
            for copy in loads(owner(step, side), 0):
                copy.start()

    if own > 1:
        for side in (1 - core, core):
            @pl.loop(0, chips)
            def _(step):
                for copy in loads(owner(step, side), 1):
                    copy.start()

    barrier = pltpu.get_barrier_semaphore()
    pl.semaphore_signal(barrier, inc=1, device_id=at_core(), device_id_type=MESH)
    for step in range(1, chips):
        pl.semaphore_signal(
            barrier, inc=1, device_id=at_chip(lax.rem(chip + step, chips)), device_id_type=MESH
        )
    for step in range(1, planes):
        pl.semaphore_signal(
            barrier, inc=1, device_id=at_plane(lax.rem(z + step, planes)), device_id_type=MESH
        )

    decay = decay_ref[...]
    own_fin[...] = over_rows(decay, jnp.ones((rows, SIZE), BF16))
    upper = jnp.logical_not(triangle(rows)) | (
        lax.broadcasted_iota(jnp.int32, (rows, rows), 0)
        == lax.broadcasted_iota(jnp.int32, (rows, rows), 1)
    )
    cumul_rows[...] = over_rows(decay, upper.astype(F32).astype(BF16))
    from_planes[z] = jnp.zeros(from_planes.shape[1:], BF16)
    pl.semaphore_wait(barrier, chips + planes - 1)

    fin_copy = remote(own_fin, core_fin, fin_s, fin_r, at_core())
    fin_copy.start()

    def make_terms(head):
        cumul = spread_column(decay, head)
        cumuls[head] = cumul
        columns = pl.ds(pl.multiple_of(head * SIZE, SIZE), SIZE)
        final = cumul[rows - 1 :, :]
        keys = (k_ref[:, columns].astype(F32) * jnp.exp(final - cumul)).astype(BF16)
        queries = (q_ref[:, columns].astype(F32) * jnp.exp(cumul)).astype(BF16)
        terms[head, 0] = over_rows(keys, v_ref[:, columns])
        terms[head, 1] = over_rows(queries, g_ref[:, columns])

    def inside(head):
        columns = pl.ds(pl.multiple_of(head * SIZE, SIZE), SIZE)
        query, key, value, grad = (ref[:, columns] for ref in (q_ref, k_ref, v_ref, g_ref))
        spread = cumuls[head] - cumul_rows[pl.ds(head, 1), :]
        weights = jnp.exp(jnp.where(triangle(rows), spread, -jnp.inf))
        probs = (over_columns(query, key) * weights).astype(BF16)
        grows = (over_columns(grad, value) * weights).astype(BF16)
        local[0, head] = jnp.dot(probs, value, preferred_element_type=F32)
        local[1, head] = jnp.dot(grows, key, preferred_element_type=F32)
        local[2, head] = over_rows(grows, query)
        local[3, head] = over_rows(probs, grad)

    chunk = heads // 8

    def inside_chunk(at):
        @pl.loop(0, chunk // 2)
        def _(pair):
            for j in range(2):
                inside(at * chunk + pair * 2 + j)

    def core_copy(i, other):
        slot = other * own + i
        head = (other * 2 + 1 - core) * own + i
        return remote(
            terms.at[head], from_core.at[slot], core_s.at[slot], core_r.at[slot], at_core()
        )

    def wait_loads(step, side):
        for copy in loads(owner(step, side), 0):
            copy.wait()

    def first(i, loading=False):
        @pl.loop(0, chips // 2)
        def _(pair):
            steps = (pair * 2, pair * 2 + 1)
            for step in steps:
                if loading:
                    wait_loads(step, 1 - core)
            for step in steps:
                make_terms(owner(step, 1 - core) * own + i)
            for step in steps:
                core_copy(i, lax.rem(chip + 1 + step, chips)).start()

    def out_copy(i, other):
        return remote(
            to_chips.at[other, i], from_chips.at[chip, i], out_s.at[other * own + i],
            out_r.at[chip * own + i], at_chip(other),
        )

    def out_arrival(i, other):
        return remote(
            to_chips.at[other, i], from_chips.at[other, i], out_s.at[other * own + i],
            out_r.at[other * own + i], at_chip(other),
        )

    def second(i, loading=False):
        @pl.loop(0, chips // 2)
        def _(pair):
            steps = (pair * 2, pair * 2 + 1)
            for step in steps:
                if loading:
                    wait_loads(step, core)
            for step in steps:
                make_terms(owner(step, core) * own + i)
            for step in steps:
                core_copy(i, lax.rem(chip + 1 + step, chips)).wait_recv()
            for step in steps:
                combine(i, step)

    def combine(i, step):
        if True:
            other = lax.rem(chip + 1 + step, chips)
            head = (other * 2 + core) * own + i
            slot = other * own + i
            mine = jnp.exp(own_fin[pl.ds(head, 1), :])
            theirs = jnp.exp(core_fin[pl.ds(head, 1), :])
            one = jnp.ones_like(mine)
            kv = (
                jnp.where(first_core, theirs, one) * terms[head, 0]
                + jnp.where(first_core, one, mine) * from_core[slot, 0]
            ).astype(BF16)
            qd = (
                jnp.where(first_core, one, theirs) * terms[head, 1]
                + jnp.where(first_core, mine, one) * from_core[slot, 1]
            ).astype(BF16)

            @pl.when(step < chips - 1)
            def _():
                to_chips[other, i, 0] = kv
                to_chips[other, i, 1] = qd
                out_copy(i, other).start()

            @pl.when(step == chips - 1)
            def _():
                from_chips[chip, i, 0] = kv
                from_chips[chip, i, 1] = qd

    first(0, True)
    fin_copy.wait_recv()
    chip_fin[chip] = own_fin[...] + core_fin[...]

    def chip_fin_copy(other, slot):
        return remote(
            chip_fin.at[chip], chip_fin.at[slot], chip_fs.at[other], chip_fr.at[slot], at_chip(other)
        )

    for step in range(1, chips):
        chip_fin_copy(lax.rem(chip + step, chips), chip).start()

    second(0, True)
    if own > 1:
        @pl.loop(0, devices)
        def _(group):
            for copy in loads(group, 1):
                copy.wait()

        @pl.loop(1, own)
        def _(i):
            first(i)
            second(i)

    for step in range(1, chips):
        other = lax.rem(chip + step, chips)
        chip_fin_copy(other, other).wait_recv()
    total = chip_fin[0]
    for other in range(1, chips):
        total = total + chip_fin[other]
    plane_fin[z] = total

    def plane_fin_copy(other, slot):
        return remote(
            plane_fin.at[z], plane_fin.at[slot], plane_fs.at[other], plane_fr.at[slot],
            at_plane(other),
        )

    for step in range(1, planes):
        plane_fin_copy(lax.rem(z + step, planes), z).start()

    def plane_copy(i, other, slot):
        kind = jnp.where(other > z, 0, 1)
        return remote(
            plane_sum.at[i, kind], from_planes.at[slot, i], plane_s.at[other * own + i],
            plane_r.at[slot * own + i], at_plane(other),
        )

    def sum_plane(i):
        head = me * own + i
        for step in range(1, chips):
            out_arrival(i, lax.rem(chip + step, chips)).wait_recv()
        kv = from_chips[0, i, 0].astype(F32)
        qd = from_chips[chips - 1, i, 1].astype(F32)
        for other in range(1, chips):
            kv = kv * jnp.exp(chip_fin[other, pl.ds(head, 1), :]) + from_chips[other, i, 0].astype(F32)
            back = chips - 1 - other
            qd = qd * jnp.exp(chip_fin[back, pl.ds(head, 1), :]) + from_chips[back, i, 1].astype(F32)
        plane_sum[i, 0] = kv.astype(BF16)
        plane_sum[i, 1] = qd.astype(BF16)
        for step in range(1, planes):
            plane_copy(i, lax.rem(z + step, planes), z).start()

    def back_copy(i, other):
        return remote(
            to_back.at[other, i], from_back.at[chip, i], back_s.at[other * own + i],
            back_r.at[chip * own + i], at_chip(other),
        )

    def back_arrival(i, other):
        return remote(
            to_back.at[other, i], from_back.at[other, i], back_s.at[other * own + i],
            back_r.at[other * own + i], at_chip(other),
        )

    def carry(i):
        head = me * own + i
        for step in range(1, planes):
            other = lax.rem(z + step, planes)
            plane_copy(i, other, other).wait_recv()
        kv = jnp.zeros((SIZE, SIZE), F32)
        qd = jnp.zeros((SIZE, SIZE), F32)
        for other in range(planes):
            factor = jnp.exp(plane_fin[other, pl.ds(head, 1), :])
            kv = jnp.where(other < z, kv * factor + from_planes[other, i].astype(F32), kv)
            back = planes - 1 - other
            factor = jnp.exp(plane_fin[back, pl.ds(head, 1), :])
            qd = jnp.where(back > z, qd * factor + from_planes[back, i].astype(F32), qd)
        for other in range(chips):
            to_back[other, i, 0] = kv.astype(BF16)
            back = chips - 1 - other
            to_back[back, i, 1] = qd.astype(BF16)
            if other < chips - 1:
                factor = jnp.exp(chip_fin[other, pl.ds(head, 1), :])
                kv = kv * factor + from_chips[other, i, 0].astype(F32)
                factor = jnp.exp(chip_fin[back, pl.ds(head, 1), :])
                qd = qd * factor + from_chips[back, i, 1].astype(F32)
        for step in range(1, chips):
            back_copy(i, lax.rem(chip + step, chips)).start()
        from_back[chip, i] = to_back[chip, i]

    def last_copy(i, other, side):
        head = (other * 2 + side) * own + i
        slot = other * own + i
        return remote(
            to_core.at[slot], states_ref.at[head], last_s.at[slot], last_r.at[slot], at_core()
        )

    def finish(i):
        @pl.loop(0, chips)
        def _(step):
            other = lax.rem(chip + step, chips)

            @pl.when(step > 0)
            def _():
                back_arrival(i, other).wait_recv()

            head = (other * 2 + core) * own + i
            slot = other * own + i
            mine = jnp.exp(own_fin[pl.ds(head, 1), :])
            theirs = jnp.exp(core_fin[pl.ds(head, 1), :])
            one = jnp.ones_like(mine)
            enter = from_back[other, i, 0].astype(F32)
            trail = from_back[other, i, 1].astype(F32)
            late = jnp.where(
                first_core, mine * enter + terms[head, 0],
                theirs * enter + from_core[slot, 0],
            )
            early = jnp.where(
                first_core, theirs * trail + from_core[slot, 1],
                mine * trail + terms[head, 1],
            )
            to_core[slot, 0] = jnp.where(first_core, late, enter).astype(BF16)
            to_core[slot, 1] = jnp.where(first_core, trail, early).astype(BF16)
            last_copy(i, other, core).start()
            states_ref[head, 0] = jnp.where(first_core, enter, late).astype(BF16)
            states_ref[head, 1] = jnp.where(first_core, early, trail).astype(BF16)

    events = []
    lead = min(3, own)
    for i in range(lead):
        events.append((sum_plane, i))
    for i in range(own):
        events.append((carry, i))
        if i + lead < own:
            events.append((sum_plane, i + lead))
    done = 0
    waited = False
    for at, (event, i) in enumerate(events):
        if event is carry and not waited:
            waited = True
            for step in range(1, planes):
                other = lax.rem(z + step, planes)
                plane_fin_copy(other, other).wait_recv()
        event(i)
        until = 8 * (at + 1) // len(events)
        for part in range(done, until):
            inside_chunk(part)
        done = until
    pl.loop(0, own)(finish)

    fin_copy.wait_send()
    for step in range(1, chips):
        chip_fin_copy(lax.rem(chip + step, chips), chip).wait_send()
    for step in range(1, planes):
        plane_fin_copy(lax.rem(z + step, planes), z).wait_send()

    @pl.loop(0, own)
    def _(i):
        @pl.loop(0, chips)
        def _(other):
            core_copy(i, other).wait_send()
            last_copy(i, other, core).wait_send()
            last_copy(i, other, 1 - core).wait_recv()

        @pl.loop(1, chips)
        def _(step):
            other = lax.rem(chip + step, chips)
            out_copy(i, other).wait_send()
            back_copy(i, other).wait_send()

        @pl.loop(1, planes)
        def _(step):
            plane_copy(i, lax.rem(z + step, planes), z).wait_send()


def carried_states(planes, devices, arrays):
    decay = arrays[-1]
    heads = decay.shape[1]
    chips, own = devices // 2, heads // devices
    square = (SIZE, SIZE)
    dma = pltpu.SemaphoreType.DMA
    slots = chips * own
    return pl.pallas_call(
        functools.partial(states_kernel, planes, devices),
        out_shape=[jax.ShapeDtypeStruct((heads, 2) + square, BF16)]
        + [jax.ShapeDtypeStruct(arrays[0].shape, BF16)] * 4
        + [
            jax.ShapeDtypeStruct((heads,) + square, F32),
            jax.ShapeDtypeStruct((4, heads) + square, F32),
        ],
        in_specs=[pl.BlockSpec(memory_space=pltpu.HBM)] * 4
        + [pl.BlockSpec(memory_space=pltpu.VMEM)],
        out_specs=[pl.BlockSpec(memory_space=pltpu.VMEM)] * 7,
        scratch_shapes=[
            pltpu.VMEM((heads, SIZE), F32),
            pltpu.VMEM((heads, 2) + square, F32),
            pltpu.VMEM((slots, 2) + square, F32),
            pltpu.VMEM((chips, own, 2) + square, BF16),
            pltpu.VMEM((chips, own, 2) + square, BF16),
            pltpu.VMEM((own, 2) + square, BF16),
            pltpu.VMEM((planes, own) + square, BF16),
            pltpu.VMEM((chips, own, 2) + square, BF16),
            pltpu.VMEM((chips, own, 2) + square, BF16),
            pltpu.VMEM((slots, 2) + square, BF16),
            pltpu.VMEM((heads, SIZE), F32),
            pltpu.VMEM((heads, SIZE), F32),
            pltpu.VMEM((chips, heads, SIZE), F32),
            pltpu.VMEM((planes, heads, SIZE), F32),
            dma((4, devices, 2)), dma, dma, dma((chips,)), dma((chips,)), dma((planes,)), dma((planes,)),
            dma((slots,)), dma((slots,)), dma((slots,)), dma((slots,)),
            dma((planes * own,)), dma((planes * own,)),
            dma((slots,)), dma((slots,)), dma((slots,)), dma((slots,)),
        ],
        compiler_params=pltpu.CompilerParams(
            collective_id=0, has_side_effects=True, vmem_limit_bytes=20 * 2**20
        ),
    )(*arrays)


def block_kernel(
    group, states_ref, q_ref, k_ref, v_ref, g_ref, cumuls, local, o_ref, dq_ref, dk_ref, dv_ref
):
    for i in range(group):
        head = pl.program_id(0) * group + i
        columns = slice(i * SIZE, (i + 1) * SIZE)
        taken = pl.ds(pl.multiple_of(head * SIZE, SIZE), SIZE)
        query, key, value, grad = (ref[:, taken] for ref in (q_ref, k_ref, v_ref, g_ref))
        enter, trail = states_ref[head, 0], states_ref[head, 1]
        cumul = cumuls[head]
        forward = jnp.exp(cumul)
        backward = jnp.exp(cumul[-1:, :] - cumul)
        o_ref[:, columns] = (
            local[0, head] + forward * jnp.dot(query, enter, preferred_element_type=F32)
        ).astype(BF16)
        dq_ref[:, columns] = (local[1, head] + forward * over_columns(grad, enter)).astype(BF16)
        dk_ref[:, columns] = (local[2, head] + backward * over_columns(value, trail)).astype(BF16)
        dv_ref[:, columns] = (
            local[3, head] + backward * jnp.dot(key, trail, preferred_element_type=F32)
        ).astype(BF16)


def block_results(held):
    rows, features = held[1].shape
    group = 4
    return pl.pallas_call(
        functools.partial(block_kernel, group),
        grid=(features // (group * SIZE),),
        out_shape=[jax.ShapeDtypeStruct((rows, features), BF16)] * 4,
        in_specs=[pl.BlockSpec(memory_space=pltpu.VMEM)] * 7,
        out_specs=[pl.BlockSpec((rows, group * SIZE), lambda i: (0, i))] * 4,
        compiler_params=pltpu.CompilerParams(vmem_limit_bytes=8 * 2**20),
    )(*held)


def solution(mesh):
    planes, devices = mesh.shape["chain"], mesh.shape["inner"]

    def shards(*arrays):
        return tuple(block_results(carried_states(planes, devices, arrays)))

    spec = P(("chain", "inner"), None)
    return jax.shard_map(
        shards, mesh=mesh, in_specs=(spec,) * 5, out_specs=(spec,) * 4, check_vma=False
    )
```

```python
import functools

import jax
import jax.numpy as jnp
from jax import lax
from jax.experimental import pallas as pl
from jax.experimental.pallas import tpu as pltpu
from jax.sharding import PartitionSpec as P

SIZE = 128
F32 = jnp.float32
BF16 = jnp.bfloat16
MESH = pl.DeviceIdType.MESH


def triangle(rows):
    row = lax.broadcasted_iota(jnp.int32, (rows, rows), 0)
    column = lax.broadcasted_iota(jnp.int32, (rows, rows), 1)
    return row >= column


def spread_columns(decay, head, count):
    rows, heads = decay.shape
    row = lax.broadcasted_iota(jnp.int32, (heads, count * SIZE), 0)
    column = lax.broadcasted_iota(jnp.int32, (heads, count * SIZE), 1)
    begin = (row - head) * SIZE
    pick = ((column >= begin) & (column < begin + SIZE)).astype(F32).astype(BF16)
    spread = jnp.dot(decay, pick, preferred_element_type=F32).astype(BF16)
    lower = triangle(rows).astype(F32).astype(BF16)
    return jnp.dot(lower, spread, preferred_element_type=F32)


def over_rows(left, right):
    return lax.dot_general(left, right, (((0,), (0,)), ((), ())), preferred_element_type=F32)


def over_columns(left, right):
    return lax.dot_general(left, right, (((1,), (1,)), ((), ())), preferred_element_type=F32)


def states_kernel(
    planes, devices, q_any, k_any, v_any, g_any, decay_ref, states_ref,
    q_ref, k_ref, v_ref, g_ref, cumuls, local,
    cumul_rows, terms, from_core, to_chips, from_chips, plane_sum, from_planes, to_back, from_back, to_core,
    own_fin, core_fin, chip_fin, plane_fin,
    load_s, fin_s, fin_r, chip_fs, chip_fr, plane_fs, plane_fr,
    core_s, core_r, out_s, out_r, plane_s, plane_r, back_s, back_r, last_s, last_r,
):
    rows, heads = decay_ref.shape
    chips = devices // 2
    own = heads // devices
    z = lax.axis_index("chain")
    me = lax.axis_index("inner")
    chip, core = me // 2, lax.rem(me, 2)
    first_core = core == 0

    def at_core():
        return (z, chip * 2 + 1 - core)

    def at_chip(other):
        return (z, other * 2 + core)

    def at_plane(other):
        return (other, me)

    def remote(src, dst, send, recv, to):
        return pltpu.make_async_remote_copy(
            src_ref=src, dst_ref=dst, send_sem=send, recv_sem=recv, device_id=to, device_id_type=MESH
        )

    def loads(group, part):
        begin, width = (0, SIZE) if part == 0 else (SIZE, (own - 1) * SIZE)
        columns = pl.ds(pl.multiple_of(group * (own * SIZE) + begin, SIZE), width)
        pairs = ((q_any, q_ref), (k_any, k_ref), (v_any, v_ref), (g_any, g_ref))
        return [
            pltpu.make_async_copy(src.at[:, columns], dst.at[:, columns], load_s.at[j, group, part])
            for j, (src, dst) in enumerate(pairs)
        ]

    def owner(step, side):
        return lax.rem(chip + 1 + step, chips) * 2 + side

    for side in (1 - core, core):
        @pl.loop(0, chips)
        def _(step):
            for copy in loads(owner(step, side), 0):
                copy.start()

    if own > 1:
        for side in (1 - core, core):
            @pl.loop(0, chips)
            def _(step):
                for copy in loads(owner(step, side), 1):
                    copy.start()

    barrier = pltpu.get_barrier_semaphore()
    pl.semaphore_signal(barrier, inc=1, device_id=at_core(), device_id_type=MESH)
    for step in range(1, chips):
        pl.semaphore_signal(
            barrier, inc=1, device_id=at_chip(lax.rem(chip + step, chips)), device_id_type=MESH
        )
    for step in range(1, planes):
        pl.semaphore_signal(
            barrier, inc=1, device_id=at_plane(lax.rem(z + step, planes)), device_id_type=MESH
        )

    decay = decay_ref[...]
    own_fin[...] = over_rows(decay, jnp.ones((rows, SIZE), BF16))
    upper = jnp.logical_not(triangle(rows)) | (
        lax.broadcasted_iota(jnp.int32, (rows, rows), 0)
        == lax.broadcasted_iota(jnp.int32, (rows, rows), 1)
    )
    cumul_rows[...] = over_rows(decay, upper.astype(F32).astype(BF16))
    @pl.loop(0, heads // 4)
    def _(group):
        spread = spread_columns(decay, group * 4, 4)
        for j in range(4):
            cumuls[group * 4 + j] = spread[:, j * SIZE : (j + 1) * SIZE]

    from_planes[z] = jnp.zeros(from_planes.shape[1:], BF16)
    pl.semaphore_wait(barrier, chips + planes - 1)

    fin_copy = remote(own_fin, core_fin, fin_s, fin_r, at_core())
    fin_copy.start()

    def make_terms(head):
        cumul = cumuls[head]
        columns = pl.ds(pl.multiple_of(head * SIZE, SIZE), SIZE)
        final = cumul[rows - 1 :, :]
        keys = (k_ref[:, columns].astype(F32) * jnp.exp(final - cumul)).astype(BF16)
        queries = (q_ref[:, columns].astype(F32) * jnp.exp(cumul)).astype(BF16)
        terms[head, 0] = over_rows(keys, v_ref[:, columns])
        terms[head, 1] = over_rows(queries, g_ref[:, columns])

    def inside(head):
        columns = pl.ds(pl.multiple_of(head * SIZE, SIZE), SIZE)
        query, key, value, grad = (ref[:, columns] for ref in (q_ref, k_ref, v_ref, g_ref))
        spread = cumuls[head] - cumul_rows[pl.ds(head, 1), :]
        weights = jnp.exp(jnp.where(triangle(rows), spread, -jnp.inf))
        probs = (over_columns(query, key) * weights).astype(BF16)
        grows = (over_columns(grad, value) * weights).astype(BF16)
        local[0, head] = jnp.dot(probs, value, preferred_element_type=F32)
        local[1, head] = jnp.dot(grows, key, preferred_element_type=F32)
        local[2, head] = over_rows(grows, query)
        local[3, head] = over_rows(probs, grad)

    chunk = heads // 8

    def inside_chunk(at):
        @pl.loop(0, chunk // 2)
        def _(pair):
            for j in range(2):
                inside(at * chunk + pair * 2 + j)

    def core_copy(i, other):
        slot = other * own + i
        head = (other * 2 + 1 - core) * own + i
        return remote(
            terms.at[head], from_core.at[slot], core_s.at[slot], core_r.at[slot], at_core()
        )

    def wait_loads(step, side):
        for copy in loads(owner(step, side), 0):
            copy.wait()

    pairs = chips // 2

    def make(i, pair):
        steps = (pair * 2, pair * 2 + 1)

        @pl.when(i == 0)
        def _():
            for step in steps:
                wait_loads(step, 1 - core)
                wait_loads(step, core)

        if own > 1:
            @pl.when((i == 1) & (pair == 0))
            def _():
                @pl.loop(0, devices)
                def _(group):
                    for copy in loads(group, 1):
                        copy.wait()

        for side in (1 - core, core):
            for step in steps:
                make_terms(owner(step, side) * own + i)
        for step in steps:
            core_copy(i, lax.rem(chip + 1 + step, chips)).start()

    def out_copy(i, other):
        return remote(
            to_chips.at[other, i], from_chips.at[chip, i], out_s.at[other * own + i],
            out_r.at[chip * own + i], at_chip(other),
        )

    def out_arrival(i, other):
        return remote(
            to_chips.at[other, i], from_chips.at[other, i], out_s.at[other * own + i],
            out_r.at[other * own + i], at_chip(other),
        )

    def combine(i, step):
        other = lax.rem(chip + 1 + step, chips)
        core_copy(i, other).wait_recv()
        head = (other * 2 + core) * own + i
        slot = other * own + i
        mine = jnp.exp(own_fin[pl.ds(head, 1), :])
        theirs = jnp.exp(core_fin[pl.ds(head, 1), :])
        one = jnp.ones_like(mine)
        kv = (
            jnp.where(first_core, theirs, one) * terms[head, 0]
            + jnp.where(first_core, one, mine) * from_core[slot, 0]
        ).astype(BF16)
        qd = (
            jnp.where(first_core, one, theirs) * terms[head, 1]
            + jnp.where(first_core, mine, one) * from_core[slot, 1]
        ).astype(BF16)

        @pl.when(step < chips - 1)
        def _():
            to_chips[other, i, 0] = kv
            to_chips[other, i, 1] = qd
            out_copy(i, other).start()

        @pl.when(step == chips - 1)
        def _():
            from_chips[chip, i, 0] = kv
            from_chips[chip, i, 1] = qd

    make(0, 0)
    fin_copy.wait_recv()
    chip_fin[chip] = own_fin[...] + core_fin[...]

    def chip_fin_copy(other, slot):
        return remote(
            chip_fin.at[chip], chip_fin.at[slot], chip_fs.at[other], chip_fr.at[slot], at_chip(other)
        )

    for step in range(1, chips):
        chip_fin_copy(lax.rem(chip + step, chips), chip).start()

    def combine_pair(i, pair):
        for step in (pair * 2, pair * 2 + 1):
            combine(i, step)

    @pl.loop(1, own * pairs)
    def _(at):
        make(at // pairs, lax.rem(at, pairs))
        combine_pair((at - 1) // pairs, lax.rem(at - 1, pairs))

    combine_pair(own - 1, pairs - 1)

    for step in range(1, chips):
        other = lax.rem(chip + step, chips)
        chip_fin_copy(other, other).wait_recv()
    total = chip_fin[0]
    for other in range(1, chips):
        total = total + chip_fin[other]
    plane_fin[z] = total

    def plane_fin_copy(other, slot):
        return remote(
            plane_fin.at[z], plane_fin.at[slot], plane_fs.at[other], plane_fr.at[slot],
            at_plane(other),
        )

    for step in range(1, planes):
        plane_fin_copy(lax.rem(z + step, planes), z).start()

    def plane_copy(i, other, slot):
        kind = jnp.where(other > z, 0, 1)
        return remote(
            plane_sum.at[i, kind], from_planes.at[slot, i], plane_s.at[other * own + i],
            plane_r.at[slot * own + i], at_plane(other),
        )

    def sum_plane(i):
        head = me * own + i
        for step in range(1, chips):
            out_arrival(i, lax.rem(chip + step, chips)).wait_recv()
        kv = from_chips[0, i, 0].astype(F32)
        qd = from_chips[chips - 1, i, 1].astype(F32)
        for other in range(1, chips):
            kv = kv * jnp.exp(chip_fin[other, pl.ds(head, 1), :]) + from_chips[other, i, 0].astype(F32)
            back = chips - 1 - other
            qd = qd * jnp.exp(chip_fin[back, pl.ds(head, 1), :]) + from_chips[back, i, 1].astype(F32)
        plane_sum[i, 0] = kv.astype(BF16)
        plane_sum[i, 1] = qd.astype(BF16)
        for step in range(1, planes):
            plane_copy(i, lax.rem(z + step, planes), z).start()

    def back_copy(i, other):
        return remote(
            to_back.at[other, i], from_back.at[chip, i], back_s.at[other * own + i],
            back_r.at[chip * own + i], at_chip(other),
        )

    def back_arrival(i, other):
        return remote(
            to_back.at[other, i], from_back.at[other, i], back_s.at[other * own + i],
            back_r.at[other * own + i], at_chip(other),
        )

    def carry(i):
        head = me * own + i
        for step in range(1, planes):
            other = lax.rem(z + step, planes)
            plane_copy(i, other, other).wait_recv()
        kv = jnp.zeros((SIZE, SIZE), F32)
        qd = jnp.zeros((SIZE, SIZE), F32)
        for other in range(planes):
            factor = jnp.exp(plane_fin[other, pl.ds(head, 1), :])
            kv = jnp.where(other < z, kv * factor + from_planes[other, i].astype(F32), kv)
            back = planes - 1 - other
            factor = jnp.exp(plane_fin[back, pl.ds(head, 1), :])
            qd = jnp.where(back > z, qd * factor + from_planes[back, i].astype(F32), qd)
        for other in range(chips):
            to_back[other, i, 0] = kv.astype(BF16)
            back = chips - 1 - other
            to_back[back, i, 1] = qd.astype(BF16)
            if other < chips - 1:
                factor = jnp.exp(chip_fin[other, pl.ds(head, 1), :])
                kv = kv * factor + from_chips[other, i, 0].astype(F32)
                factor = jnp.exp(chip_fin[back, pl.ds(head, 1), :])
                qd = qd * factor + from_chips[back, i, 1].astype(F32)
        for step in range(1, chips):
            back_copy(i, lax.rem(chip + step, chips)).start()
        from_back[chip, i] = to_back[chip, i]

    def last_copy(i, other, side):
        head = (other * 2 + side) * own + i
        slot = other * own + i
        return remote(
            to_core.at[slot], states_ref.at[head], last_s.at[slot], last_r.at[slot], at_core()
        )

    def finish(i):
        @pl.loop(0, chips)
        def _(step):
            other = lax.rem(chip + step, chips)

            @pl.when(step > 0)
            def _():
                back_arrival(i, other).wait_recv()

            head = (other * 2 + core) * own + i
            slot = other * own + i
            mine = jnp.exp(own_fin[pl.ds(head, 1), :])
            theirs = jnp.exp(core_fin[pl.ds(head, 1), :])
            one = jnp.ones_like(mine)
            enter = from_back[other, i, 0].astype(F32)
            trail = from_back[other, i, 1].astype(F32)
            late = jnp.where(
                first_core, mine * enter + terms[head, 0],
                theirs * enter + from_core[slot, 0],
            )
            early = jnp.where(
                first_core, theirs * trail + from_core[slot, 1],
                mine * trail + terms[head, 1],
            )
            to_core[slot, 0] = jnp.where(first_core, late, enter).astype(BF16)
            to_core[slot, 1] = jnp.where(first_core, trail, early).astype(BF16)
            last_copy(i, other, core).start()
            states_ref[head, 0] = jnp.where(first_core, enter, late).astype(BF16)
            states_ref[head, 1] = jnp.where(first_core, early, trail).astype(BF16)

    events = []
    lead = min(2, own)
    for i in range(lead):
        events.append((sum_plane, i))
    for i in range(own):
        events.append((carry, i))
        if i + lead < own:
            events.append((sum_plane, i + lead))
    done = 0
    waited = False
    for at, (event, i) in enumerate(events):
        if event is carry and not waited:
            waited = True
            for step in range(1, planes):
                other = lax.rem(z + step, planes)
                plane_fin_copy(other, other).wait_recv()
        event(i)
        until = 8 * (at + 1) // len(events)
        for part in range(done, until):
            inside_chunk(part)
        done = until
    pl.loop(0, own)(finish)

    fin_copy.wait_send()
    for step in range(1, chips):
        chip_fin_copy(lax.rem(chip + step, chips), chip).wait_send()
    for step in range(1, planes):
        plane_fin_copy(lax.rem(z + step, planes), z).wait_send()

    @pl.loop(0, own)
    def _(i):
        @pl.loop(0, chips)
        def _(other):
            core_copy(i, other).wait_send()
            last_copy(i, other, core).wait_send()
            last_copy(i, other, 1 - core).wait_recv()

        @pl.loop(1, chips)
        def _(step):
            other = lax.rem(chip + step, chips)
            out_copy(i, other).wait_send()
            back_copy(i, other).wait_send()

        @pl.loop(1, planes)
        def _(step):
            plane_copy(i, lax.rem(z + step, planes), z).wait_send()


def carried_states(planes, devices, arrays):
    decay = arrays[-1]
    arrays = [pltpu.with_memory_space_constraint(item, pltpu.HBM) for item in arrays[:-1]] + [decay]
    heads = decay.shape[1]
    chips, own = devices // 2, heads // devices
    square = (SIZE, SIZE)
    dma = pltpu.SemaphoreType.DMA
    slots = chips * own
    return pl.pallas_call(
        functools.partial(states_kernel, planes, devices),
        out_shape=[jax.ShapeDtypeStruct((heads, 2) + square, BF16)]
        + [jax.ShapeDtypeStruct(arrays[0].shape, BF16)] * 4
        + [
            jax.ShapeDtypeStruct((heads,) + square, F32),
            jax.ShapeDtypeStruct((4, heads) + square, F32),
        ],
        in_specs=[pl.BlockSpec(memory_space=pltpu.HBM)] * 4
        + [pl.BlockSpec(memory_space=pltpu.VMEM)],
        out_specs=[pl.BlockSpec(memory_space=pltpu.VMEM)] * 7,
        scratch_shapes=[
            pltpu.VMEM((heads, SIZE), F32),
            pltpu.VMEM((heads, 2) + square, F32),
            pltpu.VMEM((slots, 2) + square, F32),
            pltpu.VMEM((chips, own, 2) + square, BF16),
            pltpu.VMEM((chips, own, 2) + square, BF16),
            pltpu.VMEM((own, 2) + square, BF16),
            pltpu.VMEM((planes, own) + square, BF16),
            pltpu.VMEM((chips, own, 2) + square, BF16),
            pltpu.VMEM((chips, own, 2) + square, BF16),
            pltpu.VMEM((slots, 2) + square, BF16),
            pltpu.VMEM((heads, SIZE), F32),
            pltpu.VMEM((heads, SIZE), F32),
            pltpu.VMEM((chips, heads, SIZE), F32),
            pltpu.VMEM((planes, heads, SIZE), F32),
            dma((4, devices, 2)), dma, dma, dma((chips,)), dma((chips,)), dma((planes,)), dma((planes,)),
            dma((slots,)), dma((slots,)), dma((slots,)), dma((slots,)),
            dma((planes * own,)), dma((planes * own,)),
            dma((slots,)), dma((slots,)), dma((slots,)), dma((slots,)),
        ],
        compiler_params=pltpu.CompilerParams(
            collective_id=0, has_side_effects=True, vmem_limit_bytes=20 * 2**20
        ),
    )(*arrays)


def block_kernel(
    group, states_ref, q_ref, k_ref, v_ref, g_ref, cumuls, local, o_ref, dq_ref, dk_ref, dv_ref
):
    for i in range(group):
        head = pl.program_id(0) * group + i
        columns = slice(i * SIZE, (i + 1) * SIZE)
        taken = pl.ds(pl.multiple_of(head * SIZE, SIZE), SIZE)
        query, key, value, grad = (ref[:, taken] for ref in (q_ref, k_ref, v_ref, g_ref))
        enter, trail = states_ref[head, 0], states_ref[head, 1]
        cumul = cumuls[head]
        forward = jnp.exp(cumul)
        backward = jnp.exp(cumul[-1:, :] - cumul)
        o_ref[:, columns] = (
            local[0, head] + forward * jnp.dot(query, enter, preferred_element_type=F32)
        ).astype(BF16)
        dq_ref[:, columns] = (local[1, head] + forward * over_columns(grad, enter)).astype(BF16)
        dk_ref[:, columns] = (local[2, head] + backward * over_columns(value, trail)).astype(BF16)
        dv_ref[:, columns] = (
            local[3, head] + backward * jnp.dot(key, trail, preferred_element_type=F32)
        ).astype(BF16)


def block_results(held):
    rows, features = held[1].shape
    group = 4
    return pl.pallas_call(
        functools.partial(block_kernel, group),
        grid=(features // (group * SIZE),),
        out_shape=[jax.ShapeDtypeStruct((rows, features), BF16)] * 4,
        in_specs=[pl.BlockSpec(memory_space=pltpu.VMEM)] * 7,
        out_specs=[pl.BlockSpec((rows, group * SIZE), lambda i: (0, i))] * 4,
        compiler_params=pltpu.CompilerParams(vmem_limit_bytes=8 * 2**20),
    )(*held)


def solution(mesh):
    planes, devices = mesh.shape["chain"], mesh.shape["inner"]

    def shards(*arrays):
        return tuple(block_results(carried_states(planes, devices, arrays)))

    spec = P(("chain", "inner"), None)
    return jax.shard_map(
        shards, mesh=mesh, in_specs=(spec,) * 5, out_specs=(spec,) * 4, check_vma=False
    )
```

```python
import functools

import jax
import jax.numpy as jnp
from jax import lax
from jax.experimental import pallas as pl
from jax.experimental.pallas import tpu as pltpu
from jax.sharding import PartitionSpec as P

SIZE = 128
F32 = jnp.float32
BF16 = jnp.bfloat16
MESH = pl.DeviceIdType.MESH


def triangle(rows):
    row = lax.broadcasted_iota(jnp.int32, (rows, rows), 0)
    column = lax.broadcasted_iota(jnp.int32, (rows, rows), 1)
    return row >= column


def spread_columns(decay, head, count):
    rows, heads = decay.shape
    row = lax.broadcasted_iota(jnp.int32, (heads, count * SIZE), 0)
    column = lax.broadcasted_iota(jnp.int32, (heads, count * SIZE), 1)
    begin = (row - head) * SIZE
    pick = ((column >= begin) & (column < begin + SIZE)).astype(F32).astype(BF16)
    spread = jnp.dot(decay, pick, preferred_element_type=F32).astype(BF16)
    lower = triangle(rows).astype(F32).astype(BF16)
    return jnp.dot(lower, spread, preferred_element_type=F32)


def over_rows(left, right):
    return lax.dot_general(left, right, (((0,), (0,)), ((), ())), preferred_element_type=F32)


def over_columns(left, right):
    return lax.dot_general(left, right, (((1,), (1,)), ((), ())), preferred_element_type=F32)


def states_kernel(
    planes, devices, q_any, k_any, v_any, g_any, decay_ref, states_ref,
    q_ref, k_ref, v_ref, g_ref, cumuls, local,
    cumul_rows, terms, from_core, to_chips, from_chips, plane_sum, from_planes, to_back, from_back, to_core,
    own_fin, core_fin, chip_fin, plane_fin,
    load_s, fin_s, fin_r, chip_fs, chip_fr, plane_fs, plane_fr,
    core_s, core_r, out_s, out_r, plane_s, plane_r, back_s, back_r, last_s, last_r,
):
    rows, heads = decay_ref.shape
    chips = devices // 2
    own = heads // devices
    z = lax.axis_index("chain")
    me = lax.axis_index("inner")
    chip, core = me // 2, lax.rem(me, 2)
    first_core = core == 0

    def at_core():
        return (z, chip * 2 + 1 - core)

    def at_chip(other):
        return (z, other * 2 + core)

    def at_plane(other):
        return (other, me)

    def remote(src, dst, send, recv, to):
        return pltpu.make_async_remote_copy(
            src_ref=src, dst_ref=dst, send_sem=send, recv_sem=recv, device_id=to, device_id_type=MESH
        )

    def loads(group, part):
        begin, width = (0, SIZE) if part == 0 else (SIZE, (own - 1) * SIZE)
        columns = pl.ds(pl.multiple_of(group * (own * SIZE) + begin, SIZE), width)
        pairs = ((q_any, q_ref), (k_any, k_ref), (v_any, v_ref), (g_any, g_ref))
        return [
            pltpu.make_async_copy(src.at[:, columns], dst.at[:, columns], load_s.at[j, group, part])
            for j, (src, dst) in enumerate(pairs)
        ]

    def owner(step, side):
        return lax.rem(chip + 1 + step, chips) * 2 + side

    for side in (1 - core, core):
        @pl.loop(0, chips)
        def _(step):
            for copy in loads(owner(step, side), 0):
                copy.start()

    if own > 1:
        for side in (1 - core, core):
            @pl.loop(0, chips)
            def _(step):
                for copy in loads(owner(step, side), 1):
                    copy.start()

    barrier = pltpu.get_barrier_semaphore()
    pl.semaphore_signal(barrier, inc=1, device_id=at_core(), device_id_type=MESH)
    for step in range(1, chips):
        pl.semaphore_signal(
            barrier, inc=1, device_id=at_chip(lax.rem(chip + step, chips)), device_id_type=MESH
        )
    for step in range(1, planes):
        pl.semaphore_signal(
            barrier, inc=1, device_id=at_plane(lax.rem(z + step, planes)), device_id_type=MESH
        )

    decay = decay_ref[...]
    own_fin[...] = over_rows(decay, jnp.ones((rows, SIZE), BF16))
    upper = jnp.logical_not(triangle(rows)) | (
        lax.broadcasted_iota(jnp.int32, (rows, rows), 0)
        == lax.broadcasted_iota(jnp.int32, (rows, rows), 1)
    )
    cumul_rows[...] = over_rows(decay, upper.astype(F32).astype(BF16))
    @pl.loop(0, heads // 4)
    def _(group):
        spread = spread_columns(decay, group * 4, 4)
        for j in range(4):
            cumuls[group * 4 + j] = spread[:, j * SIZE : (j + 1) * SIZE]

    from_planes[z] = jnp.zeros(from_planes.shape[1:], BF16)
    pl.semaphore_wait(barrier, chips + planes - 1)

    fin_copy = remote(own_fin, core_fin, fin_s, fin_r, at_core())
    fin_copy.start()

    def make_terms(head):
        cumul = cumuls[head]
        columns = pl.ds(pl.multiple_of(head * SIZE, SIZE), SIZE)
        final = cumul[rows - 1 :, :]
        keys = (k_ref[:, columns].astype(F32) * jnp.exp(final - cumul)).astype(BF16)
        queries = (q_ref[:, columns].astype(F32) * jnp.exp(cumul)).astype(BF16)
        terms[head, 0] = over_rows(keys, v_ref[:, columns])
        terms[head, 1] = over_rows(queries, g_ref[:, columns])

    def inside(head):
        columns = pl.ds(pl.multiple_of(head * SIZE, SIZE), SIZE)
        query, key, value, grad = (ref[:, columns] for ref in (q_ref, k_ref, v_ref, g_ref))
        spread = cumuls[head] - cumul_rows[pl.ds(head, 1), :]
        weights = jnp.exp(jnp.where(triangle(rows), spread, -jnp.inf))
        probs = (over_columns(query, key) * weights).astype(BF16)
        grows = (over_columns(grad, value) * weights).astype(BF16)
        local[0, head] = jnp.dot(probs, value, preferred_element_type=F32)
        local[1, head] = jnp.dot(grows, key, preferred_element_type=F32)
        local[2, head] = over_rows(grows, query)
        local[3, head] = over_rows(probs, grad)

    chunk = heads // 8

    def inside_chunk(at):
        @pl.loop(0, chunk // 2)
        def _(pair):
            for j in range(2):
                inside(at * chunk + pair * 2 + j)

    def core_copy(i, other):
        slot = other * own + i
        head = (other * 2 + 1 - core) * own + i
        return remote(
            terms.at[head], from_core.at[slot], core_s.at[slot], core_r.at[slot], at_core()
        )

    def wait_loads(step, side):
        for copy in loads(owner(step, side), 0):
            copy.wait()

    pairs = chips // 2

    def make(i, pair):
        steps = (pair * 2, pair * 2 + 1)

        @pl.when(i == 0)
        def _():
            for step in steps:
                wait_loads(step, 1 - core)
                wait_loads(step, core)

        if own > 1:
            @pl.when((i == 1) & (pair == 0))
            def _():
                @pl.loop(0, devices)
                def _(group):
                    for copy in loads(group, 1):
                        copy.wait()

        for side in (1 - core, core):
            for step in steps:
                make_terms(owner(step, side) * own + i)
        for step in steps:
            core_copy(i, lax.rem(chip + 1 + step, chips)).start()

    def out_copy(i, other):
        return remote(
            to_chips.at[other, i], from_chips.at[chip, i], out_s.at[other * own + i],
            out_r.at[chip * own + i], at_chip(other),
        )

    def out_arrival(i, other):
        return remote(
            to_chips.at[other, i], from_chips.at[other, i], out_s.at[other * own + i],
            out_r.at[other * own + i], at_chip(other),
        )

    def combine(i, step):
        other = lax.rem(chip + 1 + step, chips)
        core_copy(i, other).wait_recv()
        head = (other * 2 + core) * own + i
        slot = other * own + i
        mine = jnp.exp(own_fin[pl.ds(head, 1), :])
        theirs = jnp.exp(core_fin[pl.ds(head, 1), :])
        one = jnp.ones_like(mine)
        kv = (
            jnp.where(first_core, theirs, one) * terms[head, 0]
            + jnp.where(first_core, one, mine) * from_core[slot, 0]
        ).astype(BF16)
        qd = (
            jnp.where(first_core, one, theirs) * terms[head, 1]
            + jnp.where(first_core, mine, one) * from_core[slot, 1]
        ).astype(BF16)

        @pl.when(step < chips - 1)
        def _():
            to_chips[other, i, 0] = kv
            to_chips[other, i, 1] = qd
            out_copy(i, other).start()

        @pl.when(step == chips - 1)
        def _():
            from_chips[chip, i, 0] = kv
            from_chips[chip, i, 1] = qd

    make(0, 0)
    fin_copy.wait_recv()
    chip_fin[chip] = own_fin[...] + core_fin[...]

    def chip_fin_copy(other, slot):
        return remote(
            chip_fin.at[chip], chip_fin.at[slot], chip_fs.at[other], chip_fr.at[slot], at_chip(other)
        )

    for step in range(1, chips):
        chip_fin_copy(lax.rem(chip + step, chips), chip).start()

    def combine_pair(i, pair):
        for step in (pair * 2, pair * 2 + 1):
            combine(i, step)

    @pl.loop(1, own * pairs)
    def _(at):
        make(at // pairs, lax.rem(at, pairs))
        combine_pair((at - 1) // pairs, lax.rem(at - 1, pairs))

    combine_pair(own - 1, pairs - 1)

    for step in range(1, chips):
        other = lax.rem(chip + step, chips)
        chip_fin_copy(other, other).wait_recv()
    total = chip_fin[0]
    for other in range(1, chips):
        total = total + chip_fin[other]
    plane_fin[z] = total

    def plane_fin_copy(other, slot):
        return remote(
            plane_fin.at[z], plane_fin.at[slot], plane_fs.at[other], plane_fr.at[slot],
            at_plane(other),
        )

    for step in range(1, planes):
        plane_fin_copy(lax.rem(z + step, planes), z).start()

    def plane_copy(i, other, slot):
        kind = jnp.where(other > z, 0, 1)
        return remote(
            plane_sum.at[i, kind], from_planes.at[slot, i], plane_s.at[other * own + i],
            plane_r.at[slot * own + i], at_plane(other),
        )

    def sum_plane(i):
        head = me * own + i
        for step in range(1, chips):
            out_arrival(i, lax.rem(chip + step, chips)).wait_recv()
        kv = from_chips[0, i, 0].astype(F32)
        qd = from_chips[chips - 1, i, 1].astype(F32)
        for other in range(1, chips):
            kv = kv * jnp.exp(chip_fin[other, pl.ds(head, 1), :]) + from_chips[other, i, 0].astype(F32)
            back = chips - 1 - other
            qd = qd * jnp.exp(chip_fin[back, pl.ds(head, 1), :]) + from_chips[back, i, 1].astype(F32)
        plane_sum[i, 0] = kv.astype(BF16)
        plane_sum[i, 1] = qd.astype(BF16)
        for step in range(1, planes):
            plane_copy(i, lax.rem(z + step, planes), z).start()

    def back_copy(i, other):
        return remote(
            to_back.at[other, i], from_back.at[chip, i], back_s.at[other * own + i],
            back_r.at[chip * own + i], at_chip(other),
        )

    def back_arrival(i, other):
        return remote(
            to_back.at[other, i], from_back.at[other, i], back_s.at[other * own + i],
            back_r.at[other * own + i], at_chip(other),
        )

    def carry(i):
        head = me * own + i
        for step in range(1, planes):
            other = lax.rem(z + step, planes)
            plane_copy(i, other, other).wait_recv()
        kv = jnp.zeros((SIZE, SIZE), F32)
        qd = jnp.zeros((SIZE, SIZE), F32)
        for other in range(planes):
            factor = jnp.exp(plane_fin[other, pl.ds(head, 1), :])
            kv = jnp.where(other < z, kv * factor + from_planes[other, i].astype(F32), kv)
            back = planes - 1 - other
            factor = jnp.exp(plane_fin[back, pl.ds(head, 1), :])
            qd = jnp.where(back > z, qd * factor + from_planes[back, i].astype(F32), qd)
        for other in range(chips):
            to_back[other, i, 0] = kv.astype(BF16)
            back = chips - 1 - other
            to_back[back, i, 1] = qd.astype(BF16)
            if other < chips - 1:
                factor = jnp.exp(chip_fin[other, pl.ds(head, 1), :])
                kv = kv * factor + from_chips[other, i, 0].astype(F32)
                factor = jnp.exp(chip_fin[back, pl.ds(head, 1), :])
                qd = qd * factor + from_chips[back, i, 1].astype(F32)
        for step in range(1, chips):
            back_copy(i, lax.rem(chip + step, chips)).start()
        from_back[chip, i] = to_back[chip, i]

    def last_copy(i, other, side):
        head = (other * 2 + side) * own + i
        slot = other * own + i
        return remote(
            to_core.at[slot], states_ref.at[head], last_s.at[slot], last_r.at[slot], at_core()
        )

    def finish(i):
        @pl.loop(0, chips)
        def _(step):
            other = lax.rem(chip + step, chips)

            @pl.when(step > 0)
            def _():
                back_arrival(i, other).wait_recv()

            head = (other * 2 + core) * own + i
            slot = other * own + i
            mine = jnp.exp(own_fin[pl.ds(head, 1), :])
            theirs = jnp.exp(core_fin[pl.ds(head, 1), :])
            one = jnp.ones_like(mine)
            enter = from_back[other, i, 0].astype(F32)
            trail = from_back[other, i, 1].astype(F32)
            late = jnp.where(
                first_core, mine * enter + terms[head, 0],
                theirs * enter + from_core[slot, 0],
            )
            early = jnp.where(
                first_core, theirs * trail + from_core[slot, 1],
                mine * trail + terms[head, 1],
            )
            to_core[slot, 0] = jnp.where(first_core, late, enter).astype(BF16)
            to_core[slot, 1] = jnp.where(first_core, trail, early).astype(BF16)
            last_copy(i, other, core).start()
            states_ref[head, 0] = jnp.where(first_core, enter, late).astype(BF16)
            states_ref[head, 1] = jnp.where(first_core, early, trail).astype(BF16)

    events = []
    lead = min(2, own)
    for i in range(lead):
        events.append((sum_plane, i))
    for i in range(own):
        events.append((carry, i))
        if i + lead < own:
            events.append((sum_plane, i + lead))
    done = 0
    waited = False
    for at, (event, i) in enumerate(events):
        if event is carry and not waited:
            waited = True
            for step in range(1, planes):
                other = lax.rem(z + step, planes)
                plane_fin_copy(other, other).wait_recv()
        event(i)
        until = 8 * (at + 1) // len(events)
        for part in range(done, until):
            inside_chunk(part)
        done = until
    pl.loop(0, own)(finish)

    fin_copy.wait_send()
    for step in range(1, chips):
        chip_fin_copy(lax.rem(chip + step, chips), chip).wait_send()
    for step in range(1, planes):
        plane_fin_copy(lax.rem(z + step, planes), z).wait_send()

    @pl.loop(0, own)
    def _(i):
        @pl.loop(0, chips)
        def _(other):
            core_copy(i, other).wait_send()
            last_copy(i, other, core).wait_send()
            last_copy(i, other, 1 - core).wait_recv()

        @pl.loop(1, chips)
        def _(step):
            other = lax.rem(chip + step, chips)
            out_copy(i, other).wait_send()
            back_copy(i, other).wait_send()

        @pl.loop(1, planes)
        def _(step):
            plane_copy(i, lax.rem(z + step, planes), z).wait_send()


def carried_states(planes, devices, arrays):
    decay = arrays[-1]
    arrays = [pltpu.with_memory_space_constraint(item, pltpu.HBM) for item in arrays[:-1]] + [decay]
    heads = decay.shape[1]
    chips, own = devices // 2, heads // devices
    square = (SIZE, SIZE)
    dma = pltpu.SemaphoreType.DMA
    slots = chips * own
    return pl.pallas_call(
        functools.partial(states_kernel, planes, devices),
        out_shape=[jax.ShapeDtypeStruct((heads, 2) + square, BF16)]
        + [jax.ShapeDtypeStruct(arrays[0].shape, BF16)] * 4
        + [
            jax.ShapeDtypeStruct((heads,) + square, F32),
            jax.ShapeDtypeStruct((4, heads) + square, F32),
        ],
        in_specs=[pl.BlockSpec(memory_space=pltpu.HBM)] * 4
        + [pl.BlockSpec(memory_space=pltpu.VMEM)],
        out_specs=[pl.BlockSpec(memory_space=pltpu.VMEM)] * 7,
        scratch_shapes=[
            pltpu.VMEM((heads, SIZE), F32),
            pltpu.VMEM((heads, 2) + square, F32),
            pltpu.VMEM((slots, 2) + square, F32),
            pltpu.VMEM((chips, own, 2) + square, BF16),
            pltpu.VMEM((chips, own, 2) + square, BF16),
            pltpu.VMEM((own, 2) + square, BF16),
            pltpu.VMEM((planes, own) + square, BF16),
            pltpu.VMEM((chips, own, 2) + square, BF16),
            pltpu.VMEM((chips, own, 2) + square, BF16),
            pltpu.VMEM((slots, 2) + square, BF16),
            pltpu.VMEM((heads, SIZE), F32),
            pltpu.VMEM((heads, SIZE), F32),
            pltpu.VMEM((chips, heads, SIZE), F32),
            pltpu.VMEM((planes, heads, SIZE), F32),
            dma((4, devices, 2)), dma, dma, dma((chips,)), dma((chips,)), dma((planes,)), dma((planes,)),
            dma((slots,)), dma((slots,)), dma((slots,)), dma((slots,)),
            dma((planes * own,)), dma((planes * own,)),
            dma((slots,)), dma((slots,)), dma((slots,)), dma((slots,)),
        ],
        compiler_params=pltpu.CompilerParams(
            collective_id=0, has_side_effects=True, vmem_limit_bytes=20 * 2**20
        ),
    )(*arrays)


def block_kernel(
    group, states_ref, q_ref, k_ref, v_ref, g_ref, cumuls, local, o_ref, dq_ref, dk_ref, dv_ref
):
    for i in range(group):
        head = pl.program_id(0) * group + i
        columns = slice(i * SIZE, (i + 1) * SIZE)
        taken = pl.ds(pl.multiple_of(head * SIZE, SIZE), SIZE)
        query, key, value, grad = (ref[:, taken] for ref in (q_ref, k_ref, v_ref, g_ref))
        enter, trail = states_ref[head, 0], states_ref[head, 1]
        cumul = cumuls[head]
        forward = jnp.exp(cumul)
        backward = jnp.exp(cumul[-1:, :] - cumul)
        o_ref[:, columns] = (
            local[0, head] + forward * jnp.dot(query, enter, preferred_element_type=F32)
        ).astype(BF16)
        dq_ref[:, columns] = (local[1, head] + forward * over_columns(grad, enter)).astype(BF16)
        dk_ref[:, columns] = (local[2, head] + backward * over_columns(value, trail)).astype(BF16)
        dv_ref[:, columns] = (
            local[3, head] + backward * jnp.dot(key, trail, preferred_element_type=F32)
        ).astype(BF16)


def block_results(held):
    rows, features = held[1].shape
    group = 8
    return pl.pallas_call(
        functools.partial(block_kernel, group),
        grid=(features // (group * SIZE),),
        out_shape=[jax.ShapeDtypeStruct((rows, features), BF16)] * 4,
        in_specs=[pl.BlockSpec(memory_space=pltpu.VMEM)] * 7,
        out_specs=[pl.BlockSpec((rows, group * SIZE), lambda i: (0, i))] * 4,
        compiler_params=pltpu.CompilerParams(vmem_limit_bytes=8 * 2**20),
    )(*held)


def solution(mesh):
    planes, devices = mesh.shape["chain"], mesh.shape["inner"]

    def shards(*arrays):
        return tuple(block_results(carried_states(planes, devices, arrays)))

    spec = P(("chain", "inner"), None)
    return jax.shard_map(
        shards, mesh=mesh, in_specs=(spec,) * 5, out_specs=(spec,) * 4, check_vma=False
    )
```
